32 devices in a mesh: row: 8 (over z, core), col: 4 (over y, x).
Axes of the slice: x: 2, y: 2, z: 4, core: 2. Of those that a mesh axis runs over, the one named last changes fastest.
Arguments:
- tensor: bfloat16 [512, 2048, 256], P(('row', 'col')), may hold values from -6 to 6
- factor_one: bfloat16 [512, 64], P(('row', 'col')), may hold values from -0.25 to 0.25
- factor_two: bfloat16 [2048, 64], P('col'), may hold values from -0.125 to 0.125
Outputs:
- gram: float32 [256, 256], replicated
The draws below stay inside these ranges and needn't reach their ends.
All inputs are finite; a program needn't handle non-finite values.
Results may differ from the reference program's by a relative error of at most 0.0003.
Values may be sent and summed in bfloat16 or wider, within the bound.
A program may use at most 64 MiB of HBM per device.

```python
import jax
import jax.numpy as jnp
from jax import lax

SLAB = 16
I2 = 2048
I3 = 256
R1 = 64
R2 = 64
I1 = 512
N_ROW = 8
N_COL = 4


def steps_of(rng, shape, cuts, least, largest):
    def one(position, shards_of):
        draws = jax.random.uniform(jax.random.fold_in(jax.random.fold_in(rng, 6), position), (shards_of,), jnp.float32, least / len(cuts), largest / len(cuts))
        return jnp.repeat(jnp.exp(draws), shape[position] // shards_of).reshape((-1,) + (1,) * (len(shape) - position - 1))

    gain = one(*cuts[0])
    for cut in cuts[1:]:
        gain = gain * one(*cut)
    return gain


def noise(key, extent, width, limit, cuts=(), held_as=jnp.bfloat16):
    entries = jax.random.normal(key, extent, jnp.float32) * width
    if len(cuts) > 0:
        entries = steps_of(key, extent, cuts, -0.22, 0.18) * entries
    return jnp.clip(entries, min=-limit, max=limit).astype(held_as)


def setup_inputs(seed: int = 0) -> dict:
    seeds = jax.random.split(jax.random.key(seed), 4)
    return {
        "tensor": noise(seeds[0], (I1, I2, I3), 1.0, 6.0, ((0, 32),)),
        "factor_one": noise(seeds[1], (I1, R1), I1 ** -0.5, 0.25, ((0, 32),)),
        "factor_two": noise(seeds[2], (I2, R2), I2 ** -0.5, 0.125, ((0, 4),)),
    }


def reference(tensor, factor_one, factor_two):
    slabs = tensor.reshape(N_ROW * N_COL, SLAB, I2, I3)
    rows_one = factor_one.reshape(N_ROW * N_COL, SLAB, R1)
    second = factor_two.astype(jnp.float32)

    def absorb(carry, pieces):
        block, first = pieces
        partly = jnp.einsum("abk,br->ark", block.astype(jnp.float32), second, precision=lax.Precision.HIGHEST)
        core = jnp.einsum("ark,as->srk", partly, first.astype(jnp.float32), precision=lax.Precision.HIGHEST)
        return carry + core, None

    start = jnp.zeros((R1, R2, I3), jnp.float32)
    core, unused = lax.scan(absorb, start, (slabs, rows_one))
    flat = core.reshape(R1 * R2, I3)
    gram = jnp.dot(flat.T, flat, precision=lax.Precision.HIGHEST, preferred_element_type=jnp.float32)
    return gram / (R1 * R2)
```

```python
import functools

import jax
import jax.numpy as jnp
from jax import lax
from jax.experimental import pallas as pl
from jax.experimental.pallas import tpu as pltpu
from jax.sharding import PartitionSpec as P

MESH = pl.DeviceIdType.MESH
F32 = jnp.float32
BF16 = jnp.bfloat16
LANES = 128
GROUP = 8
POWER = 5
TENSOR_LIMIT, ONE_LIMIT, TWO_LIMIT = 6.0, 0.25, 0.125


def split(x):
    high = x.astype(BF16)
    return high, (x - high.astype(F32)).astype(BF16)


def scale_for(bound):
    scale = 2.0 ** (125 // POWER)
    while bound > 1.0:
        bound, scale = bound / 2, scale / 2
    return scale


def dither(shape):
    places = lax.broadcasted_iota(jnp.int32, shape, 0) * 37 + lax.broadcasted_iota(jnp.int32, shape, 1) * 101
    return 1.0 + lax.rem(places, 128).astype(F32) * (2.0 ** -14 / POWER)


def encode(x, factor):
    x = x * factor
    square = x * x
    return (square * square * x).astype(BF16)


def decode(code, inverse):
    code = code.astype(F32)
    root = jnp.exp2(jnp.log2(jnp.abs(code)) * (1.0 / POWER)) * inverse
    return jnp.where(code < 0, -root, root)


def kernel(
    n_row, n_col, share,
    t_ref, f1_ref, f2_ref, out_ref,
    held, twos, ones, ones_all, spread, first, stage, sent, recv, outbox, inbox,
    part0, part1, part0_all, part1_all, total,
    load_sem, near_sem, two_send, two_recv, one_send, one_recv,
    mid_send, mid_recv, box_send, box_recv, part_send, part_recv, all_send, all_recv,
):
    slab, rank_one = f1_ref.shape
    rank_two, depth = f2_ref.shape[0], t_ref.shape[2]
    halves, chunks = sent.shape[0], sent.shape[1]
    rows = GROUP * share
    my_row, my_col = lax.axis_index("row"), lax.axis_index("col")
    half_rows = n_row // 2
    n = half_rows * n_col
    my_seat = lax.rem(my_row, half_rows)
    me = my_seat * n_col + my_col
    partner = (lax.rem(my_row + half_rows, n_row), my_col)
    pieces, block = part0.shape[0], part0.shape[1]

    for a in range(slab):
        pltpu.make_async_copy(t_ref.at[a], held.at[a], load_sem.at[a]).start()

    flips = []
    for i in range((n - 1).bit_length()):
        flips.append((1 - 2 * lax.rem(me // 2 ** i, 2)) * 2 ** i)

    def mates():
        for off in range(1, n):
            other = me
            for i, flip in enumerate(flips):
                if off >> i & 1:
                    other = other + flip
            col = lax.rem(other, n_col)
            yield other, (my_row - my_seat + (other - col) // n_col, col)

    def send(src, dst, send_sem, recv_sem, device):
        pltpu.make_async_remote_copy(
            src_ref=src, dst_ref=dst, send_sem=send_sem, recv_sem=recv_sem,
            device_id=device, device_id_type=MESH,
        ).start()

    def wait_bytes(ref, sem):
        pltpu.make_async_copy(ref, ref, sem).wait()

    cols = [(my_row, lax.rem(my_col + off, n_col)) for off in range(1, n_col)]
    lines = [(my_row - my_seat + lax.rem(my_seat + off, half_rows), my_col) for off in range(1, half_rows)]
    barrier = pltpu.get_barrier_semaphore()
    near = cols + lines + [partner]
    for device in near:
        pl.semaphore_signal(barrier, inc=1, device_id=device, device_id_type=MESH)
    twos[my_col] = f2_ref[...]
    folds = slab // GROUP
    ones[...] = jnp.concatenate([f1_ref[pl.ds(q * GROUP, GROUP), :] for q in range(folds)], axis=1)
    ones_all[me] = ones[...]
    pl.semaphore_wait(barrier, len(near))

    for device in cols:
        send(f2_ref, twos.at[my_col], two_send, two_recv, device)
    for device in lines:
        pl.semaphore_signal(near_sem, inc=1, device_id=device, device_id_type=MESH)
    factor = dither((rows, LANES))
    inverse = 1.0 / factor
    to_code = factor * scale_for(TENSOR_LIMIT * TWO_LIMIT * t_ref.shape[1])
    from_code = inverse * (1.0 / scale_for(TENSOR_LIMIT * TWO_LIMIT * t_ref.shape[1]))
    if lines:
        pl.semaphore_wait(near_sem, len(lines))
    for other, device in mates():
        send(ones, ones_all.at[me], one_send, one_recv, device)
    if cols:
        wait_bytes(twos.at[pl.ds(0, n_col - 1)], two_recv)
    second = jnp.concatenate([twos[q] for q in range(n_col)], axis=1)

    for h in range(halves):
        lanes = pl.ds(h * LANES, LANES)
        for c in range(chunks):
            for i in range(0, GROUP, 2):
                a = c * GROUP + i
                if h == 0:
                    for q in (a, a + 1):
                        pltpu.make_async_copy(t_ref.at[q], held.at[q], load_sem.at[q]).wait()
                pair = jnp.concatenate([held[a, :, lanes], held[a + 1, :, lanes]], axis=1)
                partly = jnp.dot(second, pair, preferred_element_type=F32)
                for q in range(2):
                    for b in range(n):
                        stage[b, pl.ds((i + q) * share, share), :] = partly[
                            b * share:(b + 1) * share, q * LANES:(q + 1) * LANES
                        ]
            for b in range(n):
                sent[h, c, b] = encode(stage[b], to_code)
            for other, device in mates():
                send(sent.at[h, c, other], recv.at[h, c, me], mid_send.at[h, c], mid_recv.at[h, c], device)
            recv[h, c, me] = sent[h, c, me]

    if n > 1:
        wait_bytes(ones_all.at[pl.ds(0, n - 1)], one_recv)
    packed = ones_all[...].astype(F32)
    words = spread.shape[0]
    for c in range(chunks):
        whole = packed[:, :, c * rank_one:(c + 1) * rank_one].reshape(n * GROUP, rank_one)
        per_word = LANES // rank_one
        for j in range(share):
            for w in range(words):
                cells = [whole if w * per_word + p == j else jnp.zeros_like(whole) for p in range(per_word)]
                spread[w, pl.ds(j, n * GROUP, stride=share), :] = jnp.concatenate(cells, axis=1)
        for w in range(words):
            first[c, pl.ds(w * LANES, LANES), :] = spread[w].T.astype(BF16)

    wide = dither((share * rank_one, LANES))
    core_scale = scale_for(TENSOR_LIMIT * TWO_LIMIT * t_ref.shape[1] * ONE_LIMIT * n * slab)
    core_to, core_from = wide * core_scale, (1.0 / wide) * (1.0 / core_scale)
    for h in range(halves):
        flat = None
        for c in range(chunks):
            wait_bytes(recv.at[h, c, pl.ds(0, n - 1)], mid_recv.at[h, c])
            value = decode(recv[h, c], from_code[None]).reshape(n * rows, LANES)
            high, low = split(value)
            both = jnp.dot(first[c], jnp.concatenate([high, low], axis=1), preferred_element_type=F32)
            both = both[:, :LANES] + both[:, LANES:]
            flat = both if flat is None else flat + both
        outbox[h] = encode(flat[:share * rank_one], core_to)
        send(outbox.at[h], inbox.at[h], box_send.at[h], box_recv.at[h], partner)

    mine = [decode(outbox[h], core_from) for h in range(halves)]
    turned, straight = [], []

    def product(i, j):
        (left_high, left_low), (right_high, right_low) = turned[i], straight[j]
        both = jnp.dot(left_high, jnp.concatenate([right_high, right_low], axis=1), preferred_element_type=F32)
        small = jnp.dot(left_low, right_high, preferred_element_type=F32)
        return (both[:, :LANES] + both[:, LANES:] + small).reshape(pieces, block, LANES)

    for h in range(halves):
        wait_bytes(inbox.at[h], box_recv.at[h])
        flat = mine[h] + decode(inbox[h], core_from)
        turned.append(split(flat.T))
        straight.append(split(flat))
        if h == 0:
            part0[...] = product(0, 0)
        else:
            part1[:, 0] = product(0, 1)
            part1[:, 1] = product(1, 1)
        source, landing = (part0, part0_all) if h == 0 else (part1, part1_all)
        for other, device in mates():
            @pl.when(other < pieces)
            def _():
                send(source.at[other], landing.at[me], part_send.at[h], part_recv.at[h], device)

    gain = 1.0 / (rank_one * rank_two)

    def finish():
        part0_all[me] = part0[me]
        part1_all[me] = part1[me]
        wait_bytes(part0_all.at[pl.ds(0, n - 1)], part_recv.at[0])
        total[me, 0] = jnp.sum(part0_all[...], axis=0) * gain
        wait_bytes(part1_all.at[pl.ds(0, n - 1)], part_recv.at[1])
        total[me, pl.ds(1, 2)] = jnp.sum(part1_all[...], axis=0) * gain
        for other, device in mates():
            send(total.at[me], total.at[me], all_send, all_recv, device)
        wait_bytes(part0.at[pl.ds(0, pieces - 1)], part_send.at[0])
        wait_bytes(part1.at[pl.ds(0, pieces - 1)], part_send.at[1])
        wait_bytes(total.at[pl.ds(0, pieces - 1)], all_recv)

    def follow():
        wait_bytes(part0, part_send.at[0])
        wait_bytes(part1, part_send.at[1])
        wait_bytes(total, all_recv)

    if n == pieces:
        finish()
    else:
        pl.when(me < pieces)(finish)
        pl.when(me >= pieces)(follow)

    blocks = [total[:, i].reshape(LANES, LANES) for i in range(3)]
    out_ref[:LANES, :LANES] = blocks[0]
    out_ref[:LANES, LANES:] = blocks[1]
    out_ref[LANES:, :LANES] = blocks[1].T
    out_ref[LANES:, LANES:] = blocks[2]

    if cols:
        wait_bytes(twos.at[pl.ds(0, n_col - 1)], two_send)
    wait_bytes(ones_all.at[pl.ds(0, n - 1)], one_send)
    for h in range(halves):
        for c in range(chunks):
            wait_bytes(recv.at[h, c, pl.ds(0, n - 1)], mid_send.at[h, c])
        wait_bytes(inbox.at[h], box_send.at[h])
    if n == pieces:
        wait_bytes(total.at[pl.ds(0, n - 1)], all_send)
    else:
        @pl.when(me < pieces)
        def _():
            wait_bytes(part0_all.at[pl.ds(0, n - 1)], all_send)
            wait_bytes(part1_all.at[pl.ds(0, n - 1)], all_send)


def per_device(n_row, n_col, tensor, factor_one, factor_two):
    slab, second_size, depth = tensor.shape
    rank_one, rank_two = factor_one.shape[1], factor_two.shape[1]
    n = n_row // 2 * n_col
    share = rank_two // n
    halves, chunks = depth // LANES, slab // GROUP
    rows = GROUP * share
    block = max(GROUP, LANES // n)
    pieces = LANES // block
    words = -(-share * rank_one // LANES)
    packed = (GROUP, slab // GROUP * rank_one)
    dma = pltpu.SemaphoreType.DMA
    gram = pl.pallas_call(
        functools.partial(kernel, n_row, n_col, share),
        out_shape=jax.ShapeDtypeStruct((depth, depth), F32),
        in_specs=[
            pl.BlockSpec(memory_space=pl.ANY),
            pl.BlockSpec(memory_space=pltpu.VMEM),
            pl.BlockSpec(memory_space=pltpu.VMEM),
        ],
        out_specs=pl.BlockSpec(memory_space=pltpu.VMEM),
        scratch_shapes=[
            pltpu.VMEM(tensor.shape, BF16),
            pltpu.VMEM((n_col, rank_two, second_size // n_col), BF16),
            pltpu.VMEM(packed, BF16),
            pltpu.VMEM((n, *packed), BF16),
            pltpu.VMEM((words, n * rows, LANES), F32),
            pltpu.VMEM((chunks, words * LANES, n * rows), BF16),
            pltpu.VMEM((n, rows, LANES), F32),
            pltpu.VMEM((halves, chunks, n, rows, LANES), BF16),
            pltpu.VMEM((halves, chunks, n, rows, LANES), BF16),
            pltpu.VMEM((halves, share * rank_one, LANES), BF16),
            pltpu.VMEM((halves, share * rank_one, LANES), BF16),
            pltpu.VMEM((pieces, block, LANES), F32),
            pltpu.VMEM((pieces, 2, block, LANES), F32),
            pltpu.VMEM((n, block, LANES), F32),
            pltpu.VMEM((n, 2, block, LANES), F32),
            pltpu.VMEM((pieces, 3, block, LANES), F32),
            dma((slab,)), pltpu.SemaphoreType.REGULAR,
            dma, dma, dma, dma, dma((halves, chunks)), dma((halves, chunks)),
            dma((halves,)), dma((halves,)), dma((halves,)), dma((halves,)), dma, dma,
        ],
        compiler_params=pltpu.CompilerParams(
            collective_id=0, has_side_effects=True, vmem_limit_bytes=60 * 2**20
        ),
        name="project_and_gram",
    )(tensor, factor_one, factor_two.T)
    return gram


def solution(mesh):
    sizes = mesh.shape
    placed = (P(("row", "col"), None, None), P(("row", "col"), None), P("col", None))
    return jax.shard_map(
        functools.partial(per_device, sizes["row"], sizes["col"]),
        mesh=mesh, in_specs=placed, out_specs=P(), check_vma=False,
    )
```

```python
import functools

import jax
import jax.numpy as jnp
from jax import lax
from jax.experimental import pallas as pl
from jax.experimental.pallas import tpu as pltpu
from jax.sharding import PartitionSpec as P

MESH = pl.DeviceIdType.MESH
F32 = jnp.float32
BF16 = jnp.bfloat16
LANES = 128
GROUP = 8
POWER = 5
TENSOR_LIMIT, ONE_LIMIT, TWO_LIMIT = 6.0, 0.25, 0.125


def split(x):
    high = x.astype(BF16)
    return high, (x - high.astype(F32)).astype(BF16)


def scale_for(bound):
    scale = 2.0 ** (125 // POWER)
    while bound > 1.0:
        bound, scale = bound / 2, scale / 2
    return scale


def dither(shape):
    places = lax.broadcasted_iota(jnp.int32, shape, 0) * 37 + lax.broadcasted_iota(jnp.int32, shape, 1) * 101
    return 1.0 + lax.rem(places, 128).astype(F32) * (2.0 ** -14 / POWER)


def encode(x, factor):
    x = x * factor
    square = x * x
    return (square * square * x).astype(BF16)


def decode(code, inverse):
    code = code.astype(F32)
    root = jnp.exp2(jnp.log2(jnp.abs(code)) * (1.0 / POWER)) * inverse
    return jnp.where(code < 0, -root, root)


def kernel(
    n_row, n_col, share,
    t_ref, f1_hbm, f2_hbm, out_ref,
    held, f1_ref, twos, ones, ones_all, spread, first, stage, sent, recv, outbox, inbox,
    part0, part1, part0_all, part1_all, total,
    load_sem, small_sem, near_sem, two_send, two_recv, one_send, one_recv,
    mid_send, mid_recv, box_send, box_recv, part_send, part_recv, all_send, all_recv,
):
    slab, rank_one = f1_ref.shape
    rank_two, depth = f2_hbm.shape[0], t_ref.shape[2]
    halves, groups, chunks, _, rows, _ = sent.shape
    each = share // groups
    my_row, my_col = lax.axis_index("row"), lax.axis_index("col")
    half_rows = n_row // 2
    n = half_rows * n_col
    my_seat = lax.rem(my_row, half_rows)
    me = my_seat * n_col + my_col
    partner = (lax.rem(my_row + half_rows, n_row), my_col)
    pieces, block = part0.shape[0], part0.shape[1]

    flips = []
    for i in range((n - 1).bit_length()):
        flips.append((1 - 2 * lax.rem(me // 2 ** i, 2)) * 2 ** i)

    def mates():
        for off in range(1, n):
            other = me
            for i, flip in enumerate(flips):
                if off >> i & 1:
                    other = other + flip
            col = lax.rem(other, n_col)
            yield other, (my_row - my_seat + (other - col) // n_col, col)

    def send(src, dst, send_sem, recv_sem, device):
        pltpu.make_async_remote_copy(
            src_ref=src, dst_ref=dst, send_sem=send_sem, recv_sem=recv_sem,
            device_id=device, device_id_type=MESH,
        ).start()

    def wait_bytes(ref, sem):
        pltpu.make_async_copy(ref, ref, sem).wait()

    load_two = pltpu.make_async_copy(f2_hbm, twos.at[my_col], small_sem.at[0])
    load_two.start()
    cols = [(my_row, lax.rem(my_col + off, n_col)) for off in range(1, n_col)]
    lines = [(my_row - my_seat + lax.rem(my_seat + off, half_rows), my_col) for off in range(1, half_rows)]
    barrier = pltpu.get_barrier_semaphore()
    near = cols + lines + [partner]
    for device in near:
        pl.semaphore_signal(barrier, inc=1, device_id=device, device_id_type=MESH)
    load_one = pltpu.make_async_copy(f1_hbm, f1_ref, small_sem.at[1])
    load_one.start()
    for a in range(slab):
        pltpu.make_async_copy(t_ref.at[a], held.at[a], load_sem.at[a]).start()

    load_two.wait()
    pl.semaphore_wait(barrier, len(near))
    for device in cols:
        send(twos.at[my_col], twos.at[my_col], two_send, two_recv, device)
    for device in lines:
        pl.semaphore_signal(near_sem, inc=1, device_id=device, device_id_type=MESH)
    load_one.wait()
    folds = slab // GROUP
    ones[...] = jnp.concatenate([f1_ref[pl.ds(q * GROUP, GROUP), :] for q in range(folds)], axis=1)
    ones_all[me] = ones[...]
    factor = dither((rows, LANES))
    inverse = 1.0 / factor
    to_code = factor * scale_for(TENSOR_LIMIT * TWO_LIMIT * t_ref.shape[1])
    from_code = inverse * (1.0 / scale_for(TENSOR_LIMIT * TWO_LIMIT * t_ref.shape[1]))
    if lines:
        pl.semaphore_wait(near_sem, len(lines))
    for other, device in mates():
        send(ones, ones_all.at[me], one_send, one_recv, device)
    if cols:
        wait_bytes(twos.at[pl.ds(0, n_col - 1)], two_recv)
    second = jnp.concatenate([twos[q] for q in range(n_col)], axis=1)

    def give(h, g, c):
        for b in range(n):
            sent[h, g, c, b] = encode(stage[g, c, b], to_code)
        for other, device in mates():
            send(sent.at[h, g, c, other], recv.at[h, g, c, me], mid_send.at[h, g, c], mid_recv.at[h, g, c], device)
        recv[h, g, c, me] = sent[h, g, c, me]

    for h in range(halves):
        lanes = pl.ds(h * LANES, LANES)
        for c in range(chunks):
            for i in range(0, GROUP, 2):
                a = c * GROUP + i
                if h == 0:
                    for q in (a, a + 1):
                        pltpu.make_async_copy(t_ref.at[q], held.at[q], load_sem.at[q]).wait()
                pair = jnp.concatenate([held[a, :, lanes], held[a + 1, :, lanes]], axis=1)
                partly = jnp.dot(second, pair, preferred_element_type=F32)
                for q in range(2):
                    for b in range(n):
                        for g in range(groups):
                            row = b * share + g * each
                            stage[g, c, b, pl.ds((i + q) * each, each), :] = partly[
                                row:row + each, q * LANES:(q + 1) * LANES
                            ]
            give(h, 0, c)
        for g in range(1, groups):
            for c in range(chunks):
                give(h, g, c)

    if n > 1:
        wait_bytes(ones_all.at[pl.ds(0, n - 1)], one_recv)
    packed = ones_all[...].astype(F32)
    words, per_word, span = spread.shape[0], LANES // rank_one, n * GROUP * each
    for c in range(chunks):
        whole = packed[:, :, c * rank_one:(c + 1) * rank_one].reshape(n * GROUP, rank_one)
        for j in range(each):
            for w in range(words):
                cells = [whole if w * per_word + p == j else jnp.zeros_like(whole) for p in range(per_word)]
                spread[w, pl.ds(c * span + j, n * GROUP, stride=each), :] = jnp.concatenate(cells, axis=1)
    for w in range(words):
        first[pl.ds(w * LANES, LANES), :] = spread[w].T.astype(BF16)

    wide = dither((each * rank_one, LANES))
    core_scale = scale_for(TENSOR_LIMIT * TWO_LIMIT * t_ref.shape[1] * ONE_LIMIT * n * slab)
    core_to, core_from = wide * core_scale, (1.0 / wide) * (1.0 / core_scale)
    for h in range(halves):
        for g in range(groups):
            for c in range(chunks):
                wait_bytes(recv.at[h, g, c, pl.ds(0, n - 1)], mid_recv.at[h, g, c])
            value = decode(recv[h, g].reshape(chunks * n, rows, LANES), from_code[None]).reshape(chunks * n * rows, LANES)
            both = jnp.dot(first[...], jnp.concatenate(split(value), axis=1), preferred_element_type=F32)
            core = (both[:, :LANES] + both[:, LANES:])[:each * rank_one]
            outbox[h, g] = encode(core, core_to)
            send(outbox.at[h, g], inbox.at[h, g], box_send.at[h, g], box_recv.at[h, g], partner)

    mine = [[decode(outbox[h, g], core_from) for g in range(groups)] for h in range(halves)]
    turned, straight = [], []

    def product(i, j):
        (left_high, left_low), (right_high, right_low) = turned[i], straight[j]
        both = jnp.dot(left_high, jnp.concatenate([right_high, right_low], axis=1), preferred_element_type=F32)
        small = jnp.dot(left_low, right_high, preferred_element_type=F32)
        return (both[:, :LANES] + both[:, LANES:] + small).reshape(pieces, block, LANES)

    for h in range(halves):
        parts = []
        for g in range(groups):
            wait_bytes(inbox.at[h, g], box_recv.at[h, g])
            parts.append(mine[h][g] + decode(inbox[h, g], core_from))
        flat = jnp.concatenate(parts, axis=0)
        turned.append(split(flat.T))
        straight.append(split(flat))
        if h == 0:
            part0[...] = product(0, 0)
        else:
            part1[:, 0] = product(0, 1)
            part1[:, 1] = product(1, 1)
        source, landing = (part0, part0_all) if h == 0 else (part1, part1_all)
        for other, device in mates():
            @pl.when(other < pieces)
            def _():
                send(source.at[other], landing.at[me], part_send.at[h], part_recv.at[h], device)

    gain = 1.0 / (rank_one * rank_two)

    def finish():
        part0_all[me] = part0[me]
        part1_all[me] = part1[me]
        wait_bytes(part0_all.at[pl.ds(0, n - 1)], part_recv.at[0])
        total[me, 0] = jnp.sum(part0_all[...], axis=0) * gain
        wait_bytes(part1_all.at[pl.ds(0, n - 1)], part_recv.at[1])
        total[me, pl.ds(1, 2)] = jnp.sum(part1_all[...], axis=0) * gain
        for other, device in mates():
            send(total.at[me], total.at[me], all_send, all_recv, device)
        wait_bytes(part0.at[pl.ds(0, pieces - 1)], part_send.at[0])
        wait_bytes(part1.at[pl.ds(0, pieces - 1)], part_send.at[1])
        wait_bytes(total.at[pl.ds(0, pieces - 1)], all_recv)

    def follow():
        wait_bytes(part0, part_send.at[0])
        wait_bytes(part1, part_send.at[1])
        wait_bytes(total, all_recv)

    if n == pieces:
        finish()
    else:
        pl.when(me < pieces)(finish)
        pl.when(me >= pieces)(follow)

    blocks = [total[:, i].reshape(LANES, LANES) for i in range(3)]
    out_ref[:LANES, :LANES] = blocks[0]
    out_ref[:LANES, LANES:] = blocks[1]
    out_ref[LANES:, :LANES] = blocks[1].T
    out_ref[LANES:, LANES:] = blocks[2]

    if cols:
        wait_bytes(twos.at[pl.ds(0, n_col - 1)], two_send)
    wait_bytes(ones_all.at[pl.ds(0, n - 1)], one_send)
    for h in range(halves):
        for g in range(groups):
            for c in range(chunks):
                wait_bytes(recv.at[h, g, c, pl.ds(0, n - 1)], mid_send.at[h, g, c])
            wait_bytes(inbox.at[h, g], box_send.at[h, g])
    if n == pieces:
        wait_bytes(total.at[pl.ds(0, n - 1)], all_send)
    else:
        @pl.when(me < pieces)
        def _():
            wait_bytes(part0_all.at[pl.ds(0, n - 1)], all_send)
            wait_bytes(part1_all.at[pl.ds(0, n - 1)], all_send)


def per_device(n_row, n_col, tensor, factor_one, factor_two):
    slab, second_size, depth = tensor.shape
    rank_one, rank_two = factor_one.shape[1], factor_two.shape[1]
    n = n_row // 2 * n_col
    share = rank_two // n
    halves, chunks = depth // LANES, slab // GROUP
    groups = 2 if share % 2 == 0 else 1
    each = share // groups
    rows = GROUP * each
    block = max(GROUP, LANES // n)
    pieces = LANES // block
    words = -(-each * rank_one // LANES)
    packed = (GROUP, slab // GROUP * rank_one)
    dma = pltpu.SemaphoreType.DMA
    gram = pl.pallas_call(
        functools.partial(kernel, n_row, n_col, share),
        out_shape=jax.ShapeDtypeStruct((depth, depth), F32),
        in_specs=[
            pl.BlockSpec(memory_space=pltpu.HBM),
            pl.BlockSpec(memory_space=pltpu.HBM),
            pl.BlockSpec(memory_space=pltpu.HBM),
        ],
        out_specs=pl.BlockSpec(memory_space=pltpu.VMEM),
        scratch_shapes=[
            pltpu.VMEM(tensor.shape, BF16),
            pltpu.VMEM(factor_one.shape, BF16),
            pltpu.VMEM((n_col, rank_two, second_size // n_col), BF16),
            pltpu.VMEM(packed, BF16),
            pltpu.VMEM((n, *packed), BF16),
            pltpu.VMEM((words, chunks * n * rows, LANES), F32),
            pltpu.VMEM((words * LANES, chunks * n * rows), BF16),
            pltpu.VMEM((groups, chunks, n, rows, LANES), F32),
            pltpu.VMEM((halves, groups, chunks, n, rows, LANES), BF16),
            pltpu.VMEM((halves, groups, chunks, n, rows, LANES), BF16),
            pltpu.VMEM((halves, groups, each * rank_one, LANES), BF16),
            pltpu.VMEM((halves, groups, each * rank_one, LANES), BF16),
            pltpu.VMEM((pieces, block, LANES), F32),
            pltpu.VMEM((pieces, 2, block, LANES), F32),
            pltpu.VMEM((n, block, LANES), F32),
            pltpu.VMEM((n, 2, block, LANES), F32),
            pltpu.VMEM((pieces, 3, block, LANES), F32),
            dma((slab,)), dma((2,)), pltpu.SemaphoreType.REGULAR,
            dma, dma, dma, dma, dma((halves, groups, chunks)), dma((halves, groups, chunks)),
            dma((halves, groups)), dma((halves, groups)), dma((halves,)), dma((halves,)), dma, dma,
        ],
        compiler_params=pltpu.CompilerParams(
            collective_id=0, has_side_effects=True, vmem_limit_bytes=40 * 2**20
        ),
        name="project_and_gram",
    )(*(pltpu.with_memory_space_constraint(x, pltpu.HBM) for x in (tensor, factor_one, factor_two.T)))
    return gram


def solution(mesh):
    sizes = mesh.shape
    placed = (P(("row", "col"), None, None), P(("row", "col"), None), P("col", None))
    return jax.shard_map(
        functools.partial(per_device, sizes["row"], sizes["col"]),
        mesh=mesh, in_specs=placed, out_specs=P(), check_vma=False,
    )
```

```python
import functools

import jax
import jax.numpy as jnp
from jax import lax
from jax.experimental import pallas as pl
from jax.experimental.pallas import tpu as pltpu
from jax.sharding import PartitionSpec as P

MESH = pl.DeviceIdType.MESH
F32 = jnp.float32
BF16 = jnp.bfloat16
LANES = 128
GROUP = 8
POWER = 5
TENSOR_LIMIT, ONE_LIMIT, TWO_LIMIT = 6.0, 0.25, 0.125


def split(x):
    high = x.astype(BF16)
    return high, (x - high.astype(F32)).astype(BF16)


def scale_for(bound):
    scale = 2.0 ** (125 // POWER)
    while bound > 1.0:
        bound, scale = bound / 2, scale / 2
    return scale


def dither(shape):
    places = lax.broadcasted_iota(jnp.int32, shape, 0) * 37 + lax.broadcasted_iota(jnp.int32, shape, 1) * 101
    return 1.0 + lax.rem(places, 128).astype(F32) * (2.0 ** -14 / POWER)


def encode(x, factor):
    x = x * factor
    square = x * x
    return (square * square * x).astype(BF16)


def decode(code, inverse):
    code = code.astype(F32)
    root = jnp.exp2(jnp.log2(jnp.abs(code)) * (1.0 / POWER)) * inverse
    return jnp.where(code < 0, -root, root)


def kernel(
    n_row, n_col, share,
    t_ref, f1_hbm, f2_hbm, out_ref,
    held, f1_ref, twos, ones, ones_all, first, sums, stage, sent, recv, outbox, inbox,
    part0, part1, part0_all, part1_all, total,
    load_sem, small_sem, near_sem, two_send, two_recv, one_send, one_recv,
    mid_send, mid_recv, box_send, box_recv, part_send, part_recv, all_send, all_recv,
):
    slab, rank_one = f1_ref.shape
    rank_two, depth = f2_hbm.shape[0], t_ref.shape[2]
    halves, pairs, shard = sent.shape[0], slab // 2, f2_hbm.shape[1]
    my_row, my_col = lax.axis_index("row"), lax.axis_index("col")
    half_rows = n_row // 2
    n = half_rows * n_col
    my_half = my_row // half_rows
    base = my_half * half_rows
    other_core = lambda row: row + 1 - 2 * lax.rem(row, 2)
    crossed = lambda row: row + my_half * (1 - 2 * lax.rem(row, 2))
    me = crossed(my_row - base) * n_col + my_col
    partner = (other_core(lax.rem(my_row + half_rows, n_row)), my_col)
    pieces, block = part0.shape[0], part0.shape[1]

    def flipped(place, off):
        for i in range(off.bit_length()):
            if off >> i & 1:
                place = place + (1 - 2 * lax.rem(place // 2 ** i, 2)) * 2 ** i
        return place

    def mates():
        for off in sorted(range(1, n), key=lambda off: (-(off & ~n_col).bit_count(), off // n_col % 2)):
            other = flipped(me, off)
            col = lax.rem(other, n_col)
            yield other, (base + crossed((other - col) // n_col), col)

    def send(src, dst, send_sem, recv_sem, device):
        pltpu.make_async_remote_copy(
            src_ref=src, dst_ref=dst, send_sem=send_sem, recv_sem=recv_sem,
            device_id=device, device_id_type=MESH,
        ).start()

    def wait_bytes(ref, sem):
        pltpu.make_async_copy(ref, ref, sem).wait()

    load_two = pltpu.make_async_copy(f2_hbm, twos.at[my_col], small_sem.at[0])
    load_two.start()
    offs = sorted(range(1, n_col), key=lambda off: off.bit_count())
    cols = [(my_row, flipped(my_col, off)) for off in offs]
    lines = [(base + lax.rem(my_row - base + off, half_rows), my_col) for off in range(1, half_rows)]
    barrier = pltpu.get_barrier_semaphore()
    near = cols + lines + [partner]
    for device in near:
        pl.semaphore_signal(barrier, inc=1, device_id=device, device_id_type=MESH)
    load_one = pltpu.make_async_copy(f1_hbm, f1_ref, small_sem.at[1])
    load_one.start()
    def load(a):
        return pltpu.make_async_copy(t_ref.at[a], held.at[a], load_sem.at[a])

    for a in range(slab):
        load(a).start()

    load_two.wait()
    pl.semaphore_wait(barrier, len(near))
    for i, device in enumerate(cols):
        send(twos.at[my_col], twos.at[my_col], two_send, two_recv.at[i], device)
    for device in lines:
        pl.semaphore_signal(near_sem, inc=1, device_id=device, device_id_type=MESH)
    load_one.wait()
    folds = slab // GROUP
    ones[...] = jnp.concatenate([f1_ref[pl.ds(q * GROUP, GROUP), :] for q in range(folds)], axis=1)
    ones_all[me] = ones[...]
    factor = dither((slab, LANES))
    inverse = 1.0 / factor
    to_code = factor * scale_for(TENSOR_LIMIT * TWO_LIMIT * t_ref.shape[1])
    from_code = inverse * (1.0 / scale_for(TENSOR_LIMIT * TWO_LIMIT * t_ref.shape[1]))
    if lines:
        pl.semaphore_wait(near_sem, len(lines))
    for other, device in mates():
        send(ones, ones_all.at[me], one_send, one_recv, device)

    def place(h, p, partly):
        for q in range(2):
            stage[pl.ds(2 * p + q, rank_two, stride=slab), :] = partly[:, q * LANES:(q + 1) * LANES]

    def give(h):
        for g in range(share):
            for b in range(n):
                r = b * share + g
                sent[h, r] = encode(stage[pl.ds(r * slab, slab), :], to_code)
            for other, device in mates():
                send(sent.at[h, other * share + g], recv.at[h, g, me], mid_send.at[h, g], mid_recv.at[h, g], device)
            recv[h, g, me] = sent[h, me * share + g]

    def term(q, p):
        where = pl.ds(pl.multiple_of(q * shard, shard), shard)
        pair = jnp.concatenate([held[2 * p, where, :LANES], held[2 * p + 1, where, :LANES]], axis=1)
        return jnp.dot(twos[q], pair, preferred_element_type=F32)

    shards = [my_col] + [flipped(my_col, off) for off in offs]
    split_at = pairs // 2
    for some in (range(split_at), range(split_at, pairs)):
        for i, q in enumerate(shards[:-1]):
            if i and some[0] == 0:
                wait_bytes(twos.at[q], two_recv.at[i - 1])
            for p in some:
                if i == 0:
                    load(2 * p).wait()
                    load(2 * p + 1).wait()
                sums[p] = term(q, p) if i == 0 else sums[p] + term(q, p)
    wait_bytes(twos.at[shards[-1]], two_recv.at[len(shards) - 2])
    for p in range(pairs):
        place(0, p, sums[p] + term(shards[-1], p))
    give(0)
    second = jnp.concatenate([twos[q] for q in range(n_col)], axis=1)
    for h in range(1, halves):
        lanes = pl.ds(h * LANES, LANES)
        for p in range(pairs):
            pair = jnp.concatenate([held[2 * p, :, lanes], held[2 * p + 1, :, lanes]], axis=1)
            place(h, p, jnp.dot(second, pair, preferred_element_type=F32))
        give(h)

    if n > 1:
        wait_bytes(ones_all.at[pl.ds(0, n - 1)], one_recv)
    packed = ones_all[...].astype(F32)
    whole = jnp.concatenate(
        [packed[:, :, q * rank_one:(q + 1) * rank_one] for q in range(folds)], axis=1
    ).reshape(n * slab, rank_one)
    whole = jnp.concatenate([whole, jnp.zeros((n * slab, LANES - rank_one), F32)], axis=1)
    first[...] = whole.T[:rank_one].astype(BF16)

    wide = dither((rank_one, LANES))
    core_scale = scale_for(TENSOR_LIMIT * TWO_LIMIT * t_ref.shape[1] * ONE_LIMIT * n * slab)
    core_to, core_from = wide * core_scale, (1.0 / wide) * (1.0 / core_scale)
    for h in range(halves):
        for g in range(share):
            wait_bytes(recv.at[h, g, pl.ds(0, n - 1)], mid_recv.at[h, g])
            value = decode(recv[h, g], from_code[None]).reshape(n * slab, LANES)
            both = jnp.dot(first[...], jnp.concatenate(split(value), axis=1), preferred_element_type=F32)
            outbox[h, g] = encode(both[:, :LANES] + both[:, LANES:], core_to)
            send(outbox.at[h, g], inbox.at[h, g], box_send.at[h, g], box_recv.at[h, g], partner)

    mine = [[decode(outbox[h, g], core_from) for g in range(share)] for h in range(halves)]
    turned, straight = [], []

    def product(i, j):
        (left_high, left_low), (right_high, right_low) = turned[i], straight[j]
        both = jnp.dot(left_high, jnp.concatenate([right_high, right_low], axis=1), preferred_element_type=F32)
        small = jnp.dot(left_low, right_high, preferred_element_type=F32)
        return (both[:, :LANES] + both[:, LANES:] + small).reshape(pieces, block, LANES)

    for h in range(halves):
        parts = []
        for g in range(share):
            wait_bytes(inbox.at[h, g], box_recv.at[h, g])
            parts.append(mine[h][g] + decode(inbox[h, g], core_from))
        flat = jnp.concatenate(parts, axis=0)
        turned.append(split(flat.T))
        straight.append(split(flat))
        if h == 0:
            part0[...] = product(0, 0)
        else:
            part1[:, 0] = product(0, 1)
            part1[:, 1] = product(1, 1)
        source, landing = (part0, part0_all) if h == 0 else (part1, part1_all)
        for other, device in mates():
            @pl.when(other < pieces)
            def _():
                send(source.at[other], landing.at[me], part_send.at[h], part_recv.at[h], device)

    gain = 1.0 / (rank_one * rank_two)
    parts = ((part0, part0_all, pl.ds(0, 1)), (part1, part1_all, pl.ds(1, 2)))

    def finish():
        for i, (own, every, spot) in enumerate(parts):
            every[me] = own[me]
            wait_bytes(every.at[pl.ds(0, n - 1)], part_recv.at[i])
            total[me, spot] = (jnp.sum(every[...], axis=0) * gain).reshape(-1, block, LANES)
            for other, device in mates():
                send(total.at[me, spot], total.at[me, spot], all_send.at[i], all_recv.at[i], device)
        for i, (own, every, spot) in enumerate(parts):
            wait_bytes(own.at[pl.ds(0, pieces - 1)], part_send.at[i])
            wait_bytes(own.at[pl.ds(0, pieces - 1)], all_recv.at[i])

    def follow():
        for i, (own, every, spot) in enumerate(parts):
            wait_bytes(own, part_send.at[i])
            wait_bytes(own, all_recv.at[i])

    if n == pieces:
        finish()
    else:
        pl.when(me < pieces)(finish)
        pl.when(me >= pieces)(follow)

    blocks = [total[:, i].reshape(LANES, LANES) for i in range(3)]
    out_ref[:LANES, :LANES] = blocks[0]
    out_ref[:LANES, LANES:] = blocks[1]
    out_ref[LANES:, :LANES] = blocks[1].T
    out_ref[LANES:, LANES:] = blocks[2]

    if cols:
        wait_bytes(twos.at[pl.ds(0, n_col - 1)], two_send)
    wait_bytes(ones_all.at[pl.ds(0, n - 1)], one_send)
    for h in range(halves):
        for g in range(share):
            wait_bytes(recv.at[h, g, pl.ds(0, n - 1)], mid_send.at[h, g])
            wait_bytes(inbox.at[h, g], box_send.at[h, g])

    def leave():
        for i, (own, every, spot) in enumerate(parts):
            wait_bytes(every.at[pl.ds(0, n - 1)], all_send.at[i])

    if n == pieces:
        leave()
    else:
        pl.when(me < pieces)(leave)


def per_device(n_row, n_col, tensor, factor_one, factor_two):
    slab, second_size, depth = tensor.shape
    rank_one, rank_two = factor_one.shape[1], factor_two.shape[1]
    n = n_row // 2 * n_col
    share = rank_two // n
    halves = depth // LANES
    block = max(GROUP, LANES // n)
    pieces = LANES // block
    packed = (GROUP, slab // GROUP * rank_one)
    dma = pltpu.SemaphoreType.DMA
    gram = pl.pallas_call(
        functools.partial(kernel, n_row, n_col, share),
        out_shape=jax.ShapeDtypeStruct((depth, depth), F32),
        in_specs=[
            pl.BlockSpec(memory_space=pltpu.HBM),
            pl.BlockSpec(memory_space=pltpu.HBM),
            pl.BlockSpec(memory_space=pltpu.HBM),
        ],
        out_specs=pl.BlockSpec(memory_space=pltpu.VMEM),
        scratch_shapes=[
            pltpu.VMEM(tensor.shape, BF16),
            pltpu.VMEM(factor_one.shape, BF16),
            pltpu.VMEM((n_col, rank_two, second_size // n_col), BF16),
            pltpu.VMEM(packed, BF16),
            pltpu.VMEM((n, *packed), BF16),
            pltpu.VMEM((rank_one, n * slab), BF16),
            pltpu.VMEM((slab // 2, rank_two, 2 * LANES), F32),
            pltpu.VMEM((rank_two * slab, LANES), F32),
            pltpu.VMEM((halves, rank_two, slab, LANES), BF16),
            pltpu.VMEM((halves, share, n, slab, LANES), BF16),
            pltpu.VMEM((halves, share, rank_one, LANES), BF16),
            pltpu.VMEM((halves, share, rank_one, LANES), BF16),
            pltpu.VMEM((pieces, block, LANES), F32),
            pltpu.VMEM((pieces, 2, block, LANES), F32),
            pltpu.VMEM((n, block, LANES), F32),
            pltpu.VMEM((n, 2, block, LANES), F32),
            pltpu.VMEM((pieces, 3, block, LANES), F32),
            dma((slab,)), dma((2,)), pltpu.SemaphoreType.REGULAR,
            dma, dma((n_col,)), dma, dma, dma((halves, share)), dma((halves, share)),
            dma((halves, share)), dma((halves, share)), dma((halves,)), dma((halves,)), dma((halves,)), dma((halves,)),
        ],
        compiler_params=pltpu.CompilerParams(
            collective_id=0, has_side_effects=True, vmem_limit_bytes=40 * 2**20
        ),
        name="project_and_gram",
    )(*(pltpu.with_memory_space_constraint(x, pltpu.HBM) for x in (tensor, factor_one, factor_two.T)))
    return gram


def solution(mesh):
    sizes = mesh.shape
    placed = (P(("row", "col"), None, None), P(("row", "col"), None), P("col", None))
    return jax.shard_map(
        functools.partial(per_device, sizes["row"], sizes["col"]),
        mesh=mesh, in_specs=placed, out_specs=P(), check_vma=False,
    )
```

```python
import functools

import jax
import jax.numpy as jnp
from jax import lax
from jax.experimental import pallas as pl
from jax.experimental.pallas import tpu as pltpu
from jax.sharding import PartitionSpec as P

MESH = pl.DeviceIdType.MESH
F32 = jnp.float32
BF16 = jnp.bfloat16
LANES = 128
GROUP = 8
POWER = 5
TENSOR_LIMIT, ONE_LIMIT, TWO_LIMIT = 6.0, 0.25, 0.125


def split(x):
    high = x.astype(BF16)
    return high, (x - high.astype(F32)).astype(BF16)


def scale_for(bound):
    scale = 2.0 ** (125 // POWER)
    while bound > 1.0:
        bound, scale = bound / 2, scale / 2
    return scale


def dither(shape):
    places = lax.broadcasted_iota(jnp.int32, shape, 0) * 37 + lax.broadcasted_iota(jnp.int32, shape, 1) * 101
    return 1.0 + lax.rem(places, 128).astype(F32) * (2.0 ** -14 / POWER)


def encode(x, factor):
    x = x * factor
    square = x * x
    return (square * square * x).astype(BF16)


def decode(code, inverse):
    code = code.astype(F32)
    root = jnp.exp2(jnp.log2(jnp.abs(code)) * (1.0 / POWER)) * inverse
    return jnp.where(code < 0, -root, root)


def kernel(
    n_row, n_col, share,
    t_ref, f1_hbm, f2_hbm, out_ref,
    held, f1_ref, twos, ones, ones_all, first, sums, stage, sent, recv, outbox, inbox,
    part0, part1, part0_all, part1_all, total,
    load_sem, small_sem, near_sem, two_send, two_recv, one_send, one_recv,
    mid_send, mid_recv, box_send, box_recv, part_send, part_recv, all_send, all_recv,
):
    slab, rank_one = f1_ref.shape
    rank_two, depth = f2_hbm.shape[0], t_ref.shape[2]
    halves, pairs, shard = sent.shape[0], slab // 2, f2_hbm.shape[1]
    my_row, my_col = lax.axis_index("row"), lax.axis_index("col")
    half_rows = n_row // 2
    n = half_rows * n_col
    my_half = my_row // half_rows
    base = my_half * half_rows
    other_core = lambda row: row + 1 - 2 * lax.rem(row, 2)
    crossed = lambda row: row + my_half * (1 - 2 * lax.rem(row, 2))
    me = crossed(my_row - base) * n_col + my_col
    partner = (other_core(lax.rem(my_row + half_rows, n_row)), my_col)
    pieces, block = part0.shape[0], part0.shape[1]

    def flipped(place, off):
        for i in range(off.bit_length()):
            if off >> i & 1:
                place = place + (1 - 2 * lax.rem(place // 2 ** i, 2)) * 2 ** i
        return place

    def mates():
        for off in sorted(range(1, n), key=lambda off: (-(off & ~n_col).bit_count(), off // n_col % 2)):
            other = flipped(me, off)
            col = lax.rem(other, n_col)
            yield other, (base + crossed((other - col) // n_col), col)

    def send(src, dst, send_sem, recv_sem, device):
        pltpu.make_async_remote_copy(
            src_ref=src, dst_ref=dst, send_sem=send_sem, recv_sem=recv_sem,
            device_id=device, device_id_type=MESH,
        ).start()

    def wait_bytes(ref, sem):
        pltpu.make_async_copy(ref, ref, sem).wait()

    load_two = pltpu.make_async_copy(f2_hbm, twos.at[my_col], small_sem.at[0])
    load_two.start()
    offs = sorted(range(1, n_col), key=lambda off: off.bit_count())
    cols = [(my_row, flipped(my_col, off)) for off in offs]
    lines = [(base + lax.rem(my_row - base + off, half_rows), my_col) for off in range(1, half_rows)]
    barrier = pltpu.get_barrier_semaphore()
    near = cols + lines + [partner]
    for device in near:
        pl.semaphore_signal(barrier, inc=1, device_id=device, device_id_type=MESH)
    load_one = pltpu.make_async_copy(f1_hbm, f1_ref, small_sem.at[1])
    load_one.start()
    def load(p):
        two = pl.ds(2 * p, 2)
        return pltpu.make_async_copy(t_ref.at[two], held.at[two], load_sem.at[p])

    for p in range(2):
        load(p).start()

    load_two.wait()
    pl.semaphore_wait(barrier, len(near))
    for i, device in enumerate(cols):
        send(twos.at[my_col], twos.at[my_col], two_send, two_recv.at[i], device)
    for p in range(2, pairs):
        load(p).start()
    for device in lines:
        pl.semaphore_signal(near_sem, inc=1, device_id=device, device_id_type=MESH)
    load_one.wait()
    folds = slab // GROUP
    ones[...] = jnp.concatenate([f1_ref[pl.ds(q * GROUP, GROUP), :] for q in range(folds)], axis=1)
    ones_all[me] = ones[...]
    factor = dither((slab, LANES))
    inverse = 1.0 / factor
    to_code = factor * scale_for(TENSOR_LIMIT * TWO_LIMIT * t_ref.shape[1])
    from_code = inverse * (1.0 / scale_for(TENSOR_LIMIT * TWO_LIMIT * t_ref.shape[1]))
    if lines:
        pl.semaphore_wait(near_sem, len(lines))
    for other, device in mates():
        send(ones, ones_all.at[me], one_send, one_recv, device)

    def place(h, p, partly):
        for q in range(2):
            stage[pl.ds(2 * p + q, rank_two, stride=slab), :] = partly[:, q * LANES:(q + 1) * LANES]

    def give(h):
        for g in range(share):
            for b in range(n):
                r = b * share + g
                sent[h, r] = encode(stage[pl.ds(r * slab, slab), :], to_code)
            for other, device in mates():
                send(sent.at[h, other * share + g], recv.at[h, g, me], mid_send.at[h, g], mid_recv.at[h, g], device)
            recv[h, g, me] = sent[h, me * share + g]

    def term(q, p):
        where = pl.ds(pl.multiple_of(q * shard, shard), shard)
        pair = jnp.concatenate([held[2 * p, where, :LANES], held[2 * p + 1, where, :LANES]], axis=1)
        return jnp.dot(twos[q], pair, preferred_element_type=F32)

    shards = [my_col] + [flipped(my_col, off) for off in offs]
    split_at = pairs * 3 // 4
    for some in (range(split_at), range(split_at, pairs)):
        for i, q in enumerate(shards[:-1]):
            if i and some[0] == 0:
                wait_bytes(twos.at[q], two_recv.at[i - 1])
            for p in some:
                if i == 0:
                    load(p).wait()
                sums[p] = term(q, p) if i == 0 else sums[p] + term(q, p)
    wait_bytes(twos.at[shards[-1]], two_recv.at[len(shards) - 2])
    for p in range(pairs):
        place(0, p, sums[p] + term(shards[-1], p))
    give(0)
    second = jnp.concatenate([twos[q] for q in range(n_col)], axis=1)
    for h in range(1, halves):
        lanes = pl.ds(h * LANES, LANES)
        for p in range(pairs):
            pair = jnp.concatenate([held[2 * p, :, lanes], held[2 * p + 1, :, lanes]], axis=1)
            place(h, p, jnp.dot(second, pair, preferred_element_type=F32))
        give(h)

    if n > 1:
        wait_bytes(ones_all.at[pl.ds(0, n - 1)], one_recv)
    packed = ones_all[...].astype(F32)
    whole = jnp.concatenate(
        [packed[:, :, q * rank_one:(q + 1) * rank_one] for q in range(folds)], axis=1
    ).reshape(n * slab, rank_one)
    whole = jnp.concatenate([whole, jnp.zeros((n * slab, LANES - rank_one), F32)], axis=1)
    first[...] = whole.T[:rank_one].astype(BF16)

    wide = dither((rank_one, LANES))
    core_scale = scale_for(TENSOR_LIMIT * TWO_LIMIT * t_ref.shape[1] * ONE_LIMIT * n * slab)
    core_to, core_from = wide * core_scale, (1.0 / wide) * (1.0 / core_scale)
    for h in range(halves):
        for g in range(share):
            wait_bytes(recv.at[h, g, pl.ds(0, n - 1)], mid_recv.at[h, g])
            value = decode(recv[h, g], from_code[None]).reshape(n * slab, LANES)
            both = jnp.dot(first[...], jnp.concatenate(split(value), axis=1), preferred_element_type=F32)
            outbox[h, g] = encode(both[:, :LANES] + both[:, LANES:], core_to)
            send(outbox.at[h, g], inbox.at[h, g], box_send.at[h, g], box_recv.at[h, g], partner)

    mine = [[decode(outbox[h, g], core_from) for g in range(share)] for h in range(halves)]
    turned, straight = [], []

    def product(i, j):
        (left_high, left_low), (right_high, right_low) = turned[i], straight[j]
        both = jnp.dot(left_high, jnp.concatenate([right_high, right_low], axis=1), preferred_element_type=F32)
        small = jnp.dot(left_low, right_high, preferred_element_type=F32)
        return (both[:, :LANES] + both[:, LANES:] + small).reshape(pieces, block, LANES)

    for h in range(halves):
        parts = []
        for g in range(share):
            wait_bytes(inbox.at[h, g], box_recv.at[h, g])
            parts.append(mine[h][g] + decode(inbox[h, g], core_from))
        flat = jnp.concatenate(parts, axis=0)
        turned.append(split(flat.T))
        straight.append(split(flat))
        if h == 0:
            part0[...] = product(0, 0)
        else:
            part1[:, 0] = product(0, 1)
            part1[:, 1] = product(1, 1)
        source, landing = (part0, part0_all) if h == 0 else (part1, part1_all)
        for other, device in mates():
            @pl.when(other < pieces)
            def _():
                send(source.at[other], landing.at[me], part_send.at[h], part_recv.at[h], device)

    gain = 1.0 / (rank_one * rank_two)
    parts = ((part0, part0_all, pl.ds(0, 1)), (part1, part1_all, pl.ds(1, 2)))

    def finish():
        for i, (own, every, spot) in enumerate(parts):
            every[me] = own[me]
            wait_bytes(every.at[pl.ds(0, n - 1)], part_recv.at[i])
            total[me, spot] = (jnp.sum(every[...], axis=0) * gain).reshape(-1, block, LANES)
            for other, device in mates():
                send(total.at[me, spot], total.at[me, spot], all_send.at[i], all_recv.at[i], device)
        for i, (own, every, spot) in enumerate(parts):
            wait_bytes(own.at[pl.ds(0, pieces - 1)], part_send.at[i])
            wait_bytes(own.at[pl.ds(0, pieces - 1)], all_recv.at[i])

    def follow():
        for i, (own, every, spot) in enumerate(parts):
            wait_bytes(own, part_send.at[i])
            wait_bytes(own, all_recv.at[i])

    if n == pieces:
        finish()
    else:
        pl.when(me < pieces)(finish)
        pl.when(me >= pieces)(follow)

    blocks = [total[:, i].reshape(LANES, LANES) for i in range(3)]
    out_ref[:LANES, :LANES] = blocks[0]
    out_ref[:LANES, LANES:] = blocks[1]
    out_ref[LANES:, :LANES] = blocks[1].T
    out_ref[LANES:, LANES:] = blocks[2]

    if cols:
        wait_bytes(twos.at[pl.ds(0, n_col - 1)], two_send)
    wait_bytes(ones_all.at[pl.ds(0, n - 1)], one_send)
    for h in range(halves):
        for g in range(share):
            wait_bytes(recv.at[h, g, pl.ds(0, n - 1)], mid_send.at[h, g])
            wait_bytes(inbox.at[h, g], box_send.at[h, g])

    def leave():
        for i, (own, every, spot) in enumerate(parts):
            wait_bytes(every.at[pl.ds(0, n - 1)], all_send.at[i])

    if n == pieces:
        leave()
    else:
        pl.when(me < pieces)(leave)


def per_device(n_row, n_col, tensor, factor_one, factor_two):
    slab, second_size, depth = tensor.shape
    rank_one, rank_two = factor_one.shape[1], factor_two.shape[1]
    n = n_row // 2 * n_col
    share = rank_two // n
    halves = depth // LANES
    block = max(GROUP, LANES // n)
    pieces = LANES // block
    packed = (GROUP, slab // GROUP * rank_one)
    dma = pltpu.SemaphoreType.DMA
    gram = pl.pallas_call(
        functools.partial(kernel, n_row, n_col, share),
        out_shape=jax.ShapeDtypeStruct((depth, depth), F32),
        in_specs=[
            pl.BlockSpec(memory_space=pltpu.HBM),
            pl.BlockSpec(memory_space=pltpu.HBM),
            pl.BlockSpec(memory_space=pltpu.HBM),
        ],
        out_specs=pl.BlockSpec(memory_space=pltpu.VMEM),
        scratch_shapes=[
            pltpu.VMEM(tensor.shape, BF16),
            pltpu.VMEM(factor_one.shape, BF16),
            pltpu.VMEM((n_col, rank_two, second_size // n_col), BF16),
            pltpu.VMEM(packed, BF16),
            pltpu.VMEM((n, *packed), BF16),
            pltpu.VMEM((rank_one, n * slab), BF16),
            pltpu.VMEM((slab // 2, rank_two, 2 * LANES), F32),
            pltpu.VMEM((rank_two * slab, LANES), F32),
            pltpu.VMEM((halves, rank_two, slab, LANES), BF16),
            pltpu.VMEM((halves, share, n, slab, LANES), BF16),
            pltpu.VMEM((halves, share, rank_one, LANES), BF16),
            pltpu.VMEM((halves, share, rank_one, LANES), BF16),
            pltpu.VMEM((pieces, block, LANES), F32),
            pltpu.VMEM((pieces, 2, block, LANES), F32),
            pltpu.VMEM((n, block, LANES), F32),
            pltpu.VMEM((n, 2, block, LANES), F32),
            pltpu.VMEM((pieces, 3, block, LANES), F32),
            dma((slab,)), dma((2,)), pltpu.SemaphoreType.REGULAR,
            dma, dma((n_col,)), dma, dma, dma((halves, share)), dma((halves, share)),
            dma((halves, share)), dma((halves, share)), dma((halves,)), dma((halves,)), dma((halves,)), dma((halves,)),
        ],
        compiler_params=pltpu.CompilerParams(
            collective_id=0, has_side_effects=True, vmem_limit_bytes=40 * 2**20
        ),
        name="project_and_gram",
    )(*(pltpu.with_memory_space_constraint(x, pltpu.HBM) for x in (tensor, factor_one, factor_two.T)))
    return gram


def solution(mesh):
    sizes = mesh.shape
    placed = (P(("row", "col"), None, None), P(("row", "col"), None), P("col", None))
    return jax.shard_map(
        functools.partial(per_device, sizes["row"], sizes["col"]),
        mesh=mesh, in_specs=placed, out_specs=P(), check_vma=False,
    )
```

```python
import functools

import jax
import jax.numpy as jnp
from jax import lax
from jax.experimental import pallas as pl
from jax.experimental.pallas import tpu as pltpu
from jax.sharding import PartitionSpec as P

MESH = pl.DeviceIdType.MESH
F32 = jnp.float32
BF16 = jnp.bfloat16
LANES = 128
GROUP = 8
POWER = 5
TENSOR_LIMIT, ONE_LIMIT, TWO_LIMIT = 6.0, 0.25, 0.125


def split(x):
    high = x.astype(BF16)
    return high, (x - high.astype(F32)).astype(BF16)


def scale_for(bound):
    scale = 2.0 ** (125 // POWER)
    while bound > 1.0:
        bound, scale = bound / 2, scale / 2
    return scale


def dither(shape):
    places = lax.broadcasted_iota(jnp.int32, shape, 0) * 37 + lax.broadcasted_iota(jnp.int32, shape, 1) * 101
    return 1.0 + lax.rem(places, 128).astype(F32) * (2.0 ** -14 / POWER)


def encode(x, factor):
    x = x * factor
    square = x * x
    return (square * square * x).astype(BF16)


def decode(code, inverse):
    code = code.astype(F32)
    root = jnp.exp2(jnp.log2(jnp.abs(code)) * (1.0 / POWER)) * inverse
    return jnp.where(code < 0, -root, root)


def kernel(
    n_row, n_col, share,
    t_ref, f1_hbm, f2_hbm, out_ref,
    held, f1_ref, twos, ones, ones_all, first, sums, stage, sent, recv, outbox, inbox,
    part0, part1, part0_all, part1_all, total,
    load_sem, small_sem, near_sem, two_send, two_recv, one_send, one_recv,
    mid_send, mid_recv, box_send, box_recv, part_send, part_recv, all_send, all_recv,
):
    slab, rank_one = f1_ref.shape
    rank_two, depth = f2_hbm.shape[0], t_ref.shape[2]
    halves, pairs, shard = sent.shape[0], slab // 2, f2_hbm.shape[1]
    my_row, my_col = lax.axis_index("row"), lax.axis_index("col")
    half_rows = n_row // 2
    n = half_rows * n_col
    my_half = my_row // half_rows
    base = my_half * half_rows
    other_core = lambda row: row + 1 - 2 * lax.rem(row, 2)
    crossed = lambda row: row + my_half * (half_rows - 1 - 2 * row)
    me = crossed(my_row - base) * n_col + my_col
    partner = (n_row - 1 - my_row, my_col)
    pieces, block = part0.shape[0], part0.shape[1]

    def flipped(place, off):
        for i in range(off.bit_length()):
            if off >> i & 1:
                place = place + (1 - 2 * lax.rem(place // 2 ** i, 2)) * 2 ** i
        return place

    def mates():
        for off in sorted(range(1, n), key=lambda off: (-(off & ~n_col).bit_count(), off // n_col % 2)):
            other = flipped(me, off)
            col = lax.rem(other, n_col)
            yield other, (base + crossed((other - col) // n_col), col)

    def send(src, dst, send_sem, recv_sem, device):
        pltpu.make_async_remote_copy(
            src_ref=src, dst_ref=dst, send_sem=send_sem, recv_sem=recv_sem,
            device_id=device, device_id_type=MESH,
        ).start()

    def wait_bytes(ref, sem):
        pltpu.make_async_copy(ref, ref, sem).wait()

    load_two = pltpu.make_async_copy(f2_hbm, twos.at[my_col], small_sem.at[0])
    load_two.start()
    offs = sorted(range(1, n_col), key=lambda off: off.bit_count())
    cols = [(my_row, flipped(my_col, off)) for off in offs]
    lines = [(base + lax.rem(my_row - base + off, half_rows), my_col) for off in range(1, half_rows)]
    barrier = pltpu.get_barrier_semaphore()
    near = cols + lines + [partner]
    for device in near:
        pl.semaphore_signal(barrier, inc=1, device_id=device, device_id_type=MESH)
    load_one = pltpu.make_async_copy(f1_hbm, f1_ref, small_sem.at[1])
    load_one.start()
    def load(p):
        two = pl.ds(2 * p, 2)
        return pltpu.make_async_copy(t_ref.at[two], held.at[two], load_sem.at[p])

    for p in range(2):
        load(p).start()

    load_two.wait()
    pl.semaphore_wait(barrier, len(near))
    for i, device in enumerate(cols):
        send(twos.at[my_col], twos.at[my_col], two_send, two_recv.at[i], device)
    for p in range(2, pairs):
        load(p).start()
    for device in lines:
        pl.semaphore_signal(near_sem, inc=1, device_id=device, device_id_type=MESH)
    load_one.wait()
    folds = slab // GROUP
    ones[...] = jnp.concatenate([f1_ref[pl.ds(q * GROUP, GROUP), :] for q in range(folds)], axis=1)
    ones_all[me] = ones[...]
    factor = dither((slab, LANES))
    inverse = 1.0 / factor
    to_code = factor * scale_for(TENSOR_LIMIT * TWO_LIMIT * t_ref.shape[1])
    from_code = inverse * (1.0 / scale_for(TENSOR_LIMIT * TWO_LIMIT * t_ref.shape[1]))
    if lines:
        pl.semaphore_wait(near_sem, len(lines))
    for other, device in mates():
        send(ones, ones_all.at[me], one_send, one_recv, device)

    def place(h, p, partly):
        for q in range(2):
            stage[pl.ds(2 * p + q, rank_two, stride=slab), :] = partly[:, q * LANES:(q + 1) * LANES]

    def give(h):
        for g in range(share):
            for b in range(n):
                r = b * share + g
                sent[h, r] = encode(stage[pl.ds(r * slab, slab), :], to_code)
            for other, device in mates():
                send(sent.at[h, other * share + g], recv.at[h, g, me], mid_send.at[h, g], mid_recv.at[h, g], device)
            recv[h, g, me] = sent[h, me * share + g]

    def term(q, p):
        where = pl.ds(pl.multiple_of(q * shard, shard), shard)
        pair = jnp.concatenate([held[2 * p, where, :LANES], held[2 * p + 1, where, :LANES]], axis=1)
        return jnp.dot(twos[q], pair, preferred_element_type=F32)

    shards = [my_col] + [flipped(my_col, off) for off in offs]
    split_at = pairs * 3 // 4
    for some in (range(split_at), range(split_at, pairs)):
        for i, q in enumerate(shards[:-1]):
            if i and some[0] == 0:
                wait_bytes(twos.at[q], two_recv.at[i - 1])
            for p in some:
                if i == 0:
                    load(p).wait()
                sums[p] = term(q, p) if i == 0 else sums[p] + term(q, p)
    wait_bytes(twos.at[shards[-1]], two_recv.at[len(shards) - 2])
    for p in range(pairs):
        place(0, p, sums[p] + term(shards[-1], p))
    give(0)
    second = jnp.concatenate([twos[q] for q in range(n_col)], axis=1)
    for h in range(1, halves):
        lanes = pl.ds(h * LANES, LANES)
        for p in range(pairs):
            pair = jnp.concatenate([held[2 * p, :, lanes], held[2 * p + 1, :, lanes]], axis=1)
            place(h, p, jnp.dot(second, pair, preferred_element_type=F32))
        give(h)

    if n > 1:
        wait_bytes(ones_all.at[pl.ds(0, n - 1)], one_recv)
    packed = ones_all[...].astype(F32)
    whole = jnp.concatenate(
        [packed[:, :, q * rank_one:(q + 1) * rank_one] for q in range(folds)], axis=1
    ).reshape(n * slab, rank_one)
    whole = jnp.concatenate([whole, jnp.zeros((n * slab, LANES - rank_one), F32)], axis=1)
    first[...] = whole.T[:rank_one].astype(BF16)

    wide = dither((rank_one, LANES))
    core_scale = scale_for(TENSOR_LIMIT * TWO_LIMIT * t_ref.shape[1] * ONE_LIMIT * n * slab)
    core_to, core_from = wide * core_scale, (1.0 / wide) * (1.0 / core_scale)
    for h in range(halves):
        for g in range(share):
            wait_bytes(recv.at[h, g, pl.ds(0, n - 1)], mid_recv.at[h, g])
            value = decode(recv[h, g], from_code[None]).reshape(n * slab, LANES)
            both = jnp.dot(first[...], jnp.concatenate(split(value), axis=1), preferred_element_type=F32)
            outbox[h, g] = encode(both[:, :LANES] + both[:, LANES:], core_to)
            send(outbox.at[h, g], inbox.at[h, g], box_send.at[h, g], box_recv.at[h, g], partner)

    mine = [[decode(outbox[h, g], core_from) for g in range(share)] for h in range(halves)]
    turned, straight = [], []

    def product(i, j):
        (left_high, left_low), (right_high, right_low) = turned[i], straight[j]
        both = jnp.dot(left_high, jnp.concatenate([right_high, right_low], axis=1), preferred_element_type=F32)
        small = jnp.dot(left_low, right_high, preferred_element_type=F32)
        return (both[:, :LANES] + both[:, LANES:] + small).reshape(pieces, block, LANES)

    for h in range(halves):
        parts = []
        for g in range(share):
            wait_bytes(inbox.at[h, g], box_recv.at[h, g])
            parts.append(mine[h][g] + decode(inbox[h, g], core_from))
        flat = jnp.concatenate(parts, axis=0)
        turned.append(split(flat.T))
        straight.append(split(flat))
        if h == 0:
            part0[...] = product(0, 0)
        else:
            part1[:, 0] = product(0, 1)
            part1[:, 1] = product(1, 1)
        source, landing = (part0, part0_all) if h == 0 else (part1, part1_all)
        for other, device in mates():
            @pl.when(other < pieces)
            def _():
                send(source.at[other], landing.at[me], part_send.at[h], part_recv.at[h], device)

    gain = 1.0 / (rank_one * rank_two)
    parts = ((part0, part0_all, pl.ds(0, 1)), (part1, part1_all, pl.ds(1, 2)))

    def finish():
        for i, (own, every, spot) in enumerate(parts):
            every[me] = own[me]
            wait_bytes(every.at[pl.ds(0, n - 1)], part_recv.at[i])
            total[me, spot] = (jnp.sum(every[...], axis=0) * gain).reshape(-1, block, LANES)
            for other, device in mates():
                send(total.at[me, spot], total.at[me, spot], all_send.at[i], all_recv.at[i], device)
        for i, (own, every, spot) in enumerate(parts):
            wait_bytes(own.at[pl.ds(0, pieces - 1)], part_send.at[i])
            wait_bytes(own.at[pl.ds(0, pieces - 1)], all_recv.at[i])

    def follow():
        for i, (own, every, spot) in enumerate(parts):
            wait_bytes(own, part_send.at[i])
            wait_bytes(own, all_recv.at[i])

    if n == pieces:
        finish()
    else:
        pl.when(me < pieces)(finish)
        pl.when(me >= pieces)(follow)

    blocks = [total[:, i].reshape(LANES, LANES) for i in range(3)]
    out_ref[:LANES, :LANES] = blocks[0]
    out_ref[:LANES, LANES:] = blocks[1]
    out_ref[LANES:, :LANES] = blocks[1].T
    out_ref[LANES:, LANES:] = blocks[2]

    if cols:
        wait_bytes(twos.at[pl.ds(0, n_col - 1)], two_send)
    wait_bytes(ones_all.at[pl.ds(0, n - 1)], one_send)
    for h in range(halves):
        for g in range(share):
            wait_bytes(recv.at[h, g, pl.ds(0, n - 1)], mid_send.at[h, g])
            wait_bytes(inbox.at[h, g], box_send.at[h, g])

    def leave():
        for i, (own, every, spot) in enumerate(parts):
            wait_bytes(every.at[pl.ds(0, n - 1)], all_send.at[i])

    if n == pieces:
        leave()
    else:
        pl.when(me < pieces)(leave)


def per_device(n_row, n_col, tensor, factor_one, factor_two):
    slab, second_size, depth = tensor.shape
    rank_one, rank_two = factor_one.shape[1], factor_two.shape[1]
    n = n_row // 2 * n_col
    share = rank_two // n
    halves = depth // LANES
    block = max(GROUP, LANES // n)
    pieces = LANES // block
    packed = (GROUP, slab // GROUP * rank_one)
    dma = pltpu.SemaphoreType.DMA
    gram = pl.pallas_call(
        functools.partial(kernel, n_row, n_col, share),
        out_shape=jax.ShapeDtypeStruct((depth, depth), F32),
        in_specs=[
            pl.BlockSpec(memory_space=pltpu.HBM),
            pl.BlockSpec(memory_space=pltpu.HBM),
            pl.BlockSpec(memory_space=pltpu.HBM),
        ],
        out_specs=pl.BlockSpec(memory_space=pltpu.VMEM),
        scratch_shapes=[
            pltpu.VMEM(tensor.shape, BF16),
            pltpu.VMEM(factor_one.shape, BF16),
            pltpu.VMEM((n_col, rank_two, second_size // n_col), BF16),
            pltpu.VMEM(packed, BF16),
            pltpu.VMEM((n, *packed), BF16),
            pltpu.VMEM((rank_one, n * slab), BF16),
            pltpu.VMEM((slab // 2, rank_two, 2 * LANES), F32),
            pltpu.VMEM((rank_two * slab, LANES), F32),
            pltpu.VMEM((halves, rank_two, slab, LANES), BF16),
            pltpu.VMEM((halves, share, n, slab, LANES), BF16),
            pltpu.VMEM((halves, share, rank_one, LANES), BF16),
            pltpu.VMEM((halves, share, rank_one, LANES), BF16),
            pltpu.VMEM((pieces, block, LANES), F32),
            pltpu.VMEM((pieces, 2, block, LANES), F32),
            pltpu.VMEM((n, block, LANES), F32),
            pltpu.VMEM((n, 2, block, LANES), F32),
            pltpu.VMEM((pieces, 3, block, LANES), F32),
            dma((slab,)), dma((2,)), pltpu.SemaphoreType.REGULAR,
            dma, dma((n_col,)), dma, dma, dma((halves, share)), dma((halves, share)),
            dma((halves, share)), dma((halves, share)), dma((halves,)), dma((halves,)), dma((halves,)), dma((halves,)),
        ],
        compiler_params=pltpu.CompilerParams(
            collective_id=0, has_side_effects=True, vmem_limit_bytes=40 * 2**20
        ),
        name="project_and_gram",
    )(*(pltpu.with_memory_space_constraint(x, pltpu.HBM) for x in (tensor, factor_one, factor_two.T)))
    return gram


def solution(mesh):
    sizes = mesh.shape
    placed = (P(("row", "col"), None, None), P(("row", "col"), None), P("col", None))
    return jax.shard_map(
        functools.partial(per_device, sizes["row"], sizes["col"]),
        mesh=mesh, in_specs=placed, out_specs=P(), check_vma=False,
    )
```

```python
import functools

import jax
import jax.numpy as jnp
from jax import lax
from jax.experimental import pallas as pl
from jax.experimental.pallas import tpu as pltpu
from jax.sharding import PartitionSpec as P

MESH = pl.DeviceIdType.MESH
F32 = jnp.float32
BF16 = jnp.bfloat16
LANES = 128
GROUP = 8
POWER = 5
TENSOR_LIMIT, ONE_LIMIT, TWO_LIMIT = 6.0, 0.25, 0.125


def split(x):
    high = x.astype(BF16)
    return high, (x - high.astype(F32)).astype(BF16)


def scale_for(bound):
    scale = 2.0 ** (125 // POWER)
    while bound > 1.0:
        bound, scale = bound / 2, scale / 2
    return scale


def dither(shape):
    places = lax.broadcasted_iota(jnp.int32, shape, 0) * 37 + lax.broadcasted_iota(jnp.int32, shape, 1) * 101
    return 1.0 + lax.rem(places, 128).astype(F32) * (2.0 ** -14 / POWER)


def encode(x, factor):
    x = x * factor
    square = x * x
    return (square * square * x).astype(BF16)


def decode(code, inverse):
    code = code.astype(F32)
    root = jnp.exp2(jnp.log2(jnp.abs(code)) * (1.0 / POWER)) * inverse
    return jnp.where(code < 0, -root, root)


def kernel(
    n_row, n_col, share,
    t_ref, f1_hbm, f2_hbm, out_ref,
    held, f1_ref, twos, ones, ones_all, first, sums, stage, sent, recv, outbox, inbox,
    part0, part1, part0_all, part1_all, total,
    load_sem, small_sem, near_sem, two_send, two_recv, one_send, one_recv,
    mid_send, mid_recv, box_send, box_recv, part_send, part_recv, all_send, all_recv,
):
    slab, rank_one = f1_ref.shape
    rank_two, depth = f2_hbm.shape[0], t_ref.shape[2]
    halves, pairs, shard = sent.shape[0], slab // 2, f2_hbm.shape[1]
    my_row, my_col = lax.axis_index("row"), lax.axis_index("col")
    half_rows = n_row // 2
    n = half_rows * n_col
    my_half = my_row // half_rows
    base = my_half * half_rows
    other_core = lambda row: row + 1 - 2 * lax.rem(row, 2)
    crossed = lambda row: row + my_half * (half_rows - 1 - 2 * row)
    me = crossed(my_row - base) * n_col + my_col
    partner = (n_row - 1 - my_row, my_col)
    pieces, block = part0.shape[0], part0.shape[1]

    def flipped(place, off):
        for i in range(off.bit_length()):
            if off >> i & 1:
                place = place + (1 - 2 * lax.rem(place // 2 ** i, 2)) * 2 ** i
        return place

    def mates():
        for off in sorted(range(1, n), key=lambda off: (-(off & ~n_col).bit_count(), 1 - off // n_col % 2)):
            other = flipped(me, off)
            col = lax.rem(other, n_col)
            yield other, (base + crossed((other - col) // n_col), col)

    def send(src, dst, send_sem, recv_sem, device):
        pltpu.make_async_remote_copy(
            src_ref=src, dst_ref=dst, send_sem=send_sem, recv_sem=recv_sem,
            device_id=device, device_id_type=MESH,
        ).start()

    def wait_bytes(ref, sem):
        pltpu.make_async_copy(ref, ref, sem).wait()

    load_two = pltpu.make_async_copy(f2_hbm, twos.at[my_col], small_sem.at[0])
    load_two.start()
    offs = sorted(range(1, n_col), key=lambda off: off.bit_count())
    cols = [(my_row, flipped(my_col, off)) for off in offs]
    lines = [(base + lax.rem(my_row - base + off, half_rows), my_col) for off in range(1, half_rows)]
    barrier = pltpu.get_barrier_semaphore()
    near = cols + lines + [partner]
    for device in near:
        pl.semaphore_signal(barrier, inc=1, device_id=device, device_id_type=MESH)
    load_one = pltpu.make_async_copy(f1_hbm, f1_ref, small_sem.at[1])
    load_one.start()
    def load(p):
        two = pl.ds(2 * p, 2)
        return pltpu.make_async_copy(t_ref.at[two], held.at[two], load_sem.at[p])

    for p in range(4):
        load(p).start()

    load_two.wait()
    pl.semaphore_wait(barrier, len(near))
    for i, device in enumerate(cols):
        send(twos.at[my_col], twos.at[my_col], two_send, two_recv.at[i], device)
    for p in range(4, pairs):
        load(p).start()
    for device in lines:
        pl.semaphore_signal(near_sem, inc=1, device_id=device, device_id_type=MESH)
    load_one.wait()
    folds = slab // GROUP
    ones[...] = jnp.concatenate([f1_ref[pl.ds(q * GROUP, GROUP), :] for q in range(folds)], axis=1)
    ones_all[me] = ones[...]
    factor = dither((slab, LANES))
    inverse = 1.0 / factor
    to_code = factor * scale_for(TENSOR_LIMIT * TWO_LIMIT * t_ref.shape[1])
    from_code = inverse * (1.0 / scale_for(TENSOR_LIMIT * TWO_LIMIT * t_ref.shape[1]))
    if lines:
        pl.semaphore_wait(near_sem, len(lines))
    for other, device in mates():
        send(ones, ones_all.at[me], one_send, one_recv, device)

    def place(h, p, partly):
        for q in range(2):
            stage[pl.ds(2 * p + q, rank_two, stride=slab), :] = partly[:, q * LANES:(q + 1) * LANES]

    def give(h):
        for g in range(share):
            for b in range(n):
                r = b * share + g
                sent[h, r] = encode(stage[pl.ds(r * slab, slab), :], to_code)
            for other, device in mates():
                send(sent.at[h, other * share + g], recv.at[h, g, me], mid_send.at[h, g], mid_recv.at[h, g], device)
            recv[h, g, me] = sent[h, me * share + g]

    def term(q, p):
        where = pl.ds(pl.multiple_of(q * shard, shard), shard)
        pair = jnp.concatenate([held[2 * p, where, :LANES], held[2 * p + 1, where, :LANES]], axis=1)
        return jnp.dot(twos[q], pair, preferred_element_type=F32)

    shards = [my_col] + [flipped(my_col, off) for off in offs]
    split_at = pairs * 3 // 4
    for some in (range(split_at), range(split_at, pairs)):
        for i, q in enumerate(shards[:-1]):
            if i and some[0] == 0:
                wait_bytes(twos.at[q], two_recv.at[i - 1])
            for p in some:
                if i == 0:
                    load(p).wait()
                sums[p] = term(q, p) if i == 0 else sums[p] + term(q, p)
    wait_bytes(twos.at[shards[-1]], two_recv.at[len(shards) - 2])
    for p in range(pairs):
        place(0, p, sums[p] + term(shards[-1], p))
    give(0)
    second = jnp.concatenate([twos[q] for q in range(n_col)], axis=1)
    for h in range(1, halves):
        lanes = pl.ds(h * LANES, LANES)
        for p in range(pairs):
            pair = jnp.concatenate([held[2 * p, :, lanes], held[2 * p + 1, :, lanes]], axis=1)
            place(h, p, jnp.dot(second, pair, preferred_element_type=F32))
        give(h)

    if n > 1:
        wait_bytes(ones_all.at[pl.ds(0, n - 1)], one_recv)
    packed = ones_all[...].astype(F32)
    whole = jnp.concatenate(
        [packed[:, :, q * rank_one:(q + 1) * rank_one] for q in range(folds)], axis=1
    ).reshape(n * slab, rank_one)
    whole = jnp.concatenate([whole, jnp.zeros((n * slab, LANES - rank_one), F32)], axis=1)
    first[...] = whole.T[:rank_one].astype(BF16)

    wide = dither((rank_one, LANES))
    core_scale = scale_for(TENSOR_LIMIT * TWO_LIMIT * t_ref.shape[1] * ONE_LIMIT * n * slab)
    core_to, core_from = wide * core_scale, (1.0 / wide) * (1.0 / core_scale)
    for h in range(halves):
        for g in range(share):
            wait_bytes(recv.at[h, g, pl.ds(0, n - 1)], mid_recv.at[h, g])
            value = decode(recv[h, g], from_code[None]).reshape(n * slab, LANES)
            both = jnp.dot(first[...], jnp.concatenate(split(value), axis=1), preferred_element_type=F32)
            outbox[h, g] = encode(both[:, :LANES] + both[:, LANES:], core_to)
            send(outbox.at[h, g], inbox.at[h, g], box_send.at[h, g], box_recv.at[h, g], partner)

    mine = [[decode(outbox[h, g], core_from) for g in range(share)] for h in range(halves)]
    turned, straight = [], []

    def product(i, j):
        (left_high, left_low), (right_high, right_low) = turned[i], straight[j]
        both = jnp.dot(left_high, jnp.concatenate([right_high, right_low], axis=1), preferred_element_type=F32)
        small = jnp.dot(left_low, right_high, preferred_element_type=F32)
        return (both[:, :LANES] + both[:, LANES:] + small).reshape(pieces, block, LANES)

    for h in range(halves):
        parts = []
        for g in range(share):
            wait_bytes(inbox.at[h, g], box_recv.at[h, g])
            parts.append(mine[h][g] + decode(inbox[h, g], core_from))
        flat = jnp.concatenate(parts, axis=0)
        turned.append(split(flat.T))
        straight.append(split(flat))
        if h == 0:
            part0[...] = product(0, 0)
        else:
            part1[:, 0] = product(0, 1)
            part1[:, 1] = product(1, 1)
        source, landing = (part0, part0_all) if h == 0 else (part1, part1_all)
        for other, device in mates():
            @pl.when(other < pieces)
            def _():
                send(source.at[other], landing.at[me], part_send.at[h], part_recv.at[h], device)

    gain = 1.0 / (rank_one * rank_two)
    parts = ((part0, part0_all, pl.ds(0, 1)), (part1, part1_all, pl.ds(1, 2)))

    def finish():
        for i, (own, every, spot) in enumerate(parts):
            every[me] = own[me]
            wait_bytes(every.at[pl.ds(0, n - 1)], part_recv.at[i])
            total[me, spot] = (jnp.sum(every[...], axis=0) * gain).reshape(-1, block, LANES)
            for other, device in mates():
                send(total.at[me, spot], total.at[me, spot], all_send.at[i], all_recv.at[i], device)
        for i, (own, every, spot) in enumerate(parts):
            wait_bytes(own.at[pl.ds(0, pieces - 1)], part_send.at[i])
            wait_bytes(own.at[pl.ds(0, pieces - 1)], all_recv.at[i])

    def follow():
        for i, (own, every, spot) in enumerate(parts):
            wait_bytes(own, part_send.at[i])
            wait_bytes(own, all_recv.at[i])

    if n == pieces:
        finish()
    else:
        pl.when(me < pieces)(finish)
        pl.when(me >= pieces)(follow)

    blocks = [total[:, i].reshape(LANES, LANES) for i in range(3)]
    out_ref[:LANES, :LANES] = blocks[0]
    out_ref[:LANES, LANES:] = blocks[1]
    out_ref[LANES:, :LANES] = blocks[1].T
    out_ref[LANES:, LANES:] = blocks[2]

    if cols:
        wait_bytes(twos.at[pl.ds(0, n_col - 1)], two_send)
    wait_bytes(ones_all.at[pl.ds(0, n - 1)], one_send)
    for h in range(halves):
        for g in range(share):
            wait_bytes(recv.at[h, g, pl.ds(0, n - 1)], mid_send.at[h, g])
            wait_bytes(inbox.at[h, g], box_send.at[h, g])

    def leave():
        for i, (own, every, spot) in enumerate(parts):
            wait_bytes(every.at[pl.ds(0, n - 1)], all_send.at[i])

    if n == pieces:
        leave()
    else:
        pl.when(me < pieces)(leave)


def per_device(n_row, n_col, tensor, factor_one, factor_two):
    slab, second_size, depth = tensor.shape
    rank_one, rank_two = factor_one.shape[1], factor_two.shape[1]
    n = n_row // 2 * n_col
    share = rank_two // n
    halves = depth // LANES
    block = max(GROUP, LANES // n)
    pieces = LANES // block
    packed = (GROUP, slab // GROUP * rank_one)
    dma = pltpu.SemaphoreType.DMA
    gram = pl.pallas_call(
        functools.partial(kernel, n_row, n_col, share),
        out_shape=jax.ShapeDtypeStruct((depth, depth), F32),
        in_specs=[
            pl.BlockSpec(memory_space=pltpu.HBM),
            pl.BlockSpec(memory_space=pltpu.HBM),
            pl.BlockSpec(memory_space=pltpu.HBM),
        ],
        out_specs=pl.BlockSpec(memory_space=pltpu.VMEM),
        scratch_shapes=[
            pltpu.VMEM(tensor.shape, BF16),
            pltpu.VMEM(factor_one.shape, BF16),
            pltpu.VMEM((n_col, rank_two, second_size // n_col), BF16),
            pltpu.VMEM(packed, BF16),
            pltpu.VMEM((n, *packed), BF16),
            pltpu.VMEM((rank_one, n * slab), BF16),
            pltpu.VMEM((slab // 2, rank_two, 2 * LANES), F32),
            pltpu.VMEM((rank_two * slab, LANES), F32),
            pltpu.VMEM((halves, rank_two, slab, LANES), BF16),
            pltpu.VMEM((halves, share, n, slab, LANES), BF16),
            pltpu.VMEM((halves, share, rank_one, LANES), BF16),
            pltpu.VMEM((halves, share, rank_one, LANES), BF16),
            pltpu.VMEM((pieces, block, LANES), F32),
            pltpu.VMEM((pieces, 2, block, LANES), F32),
            pltpu.VMEM((n, block, LANES), F32),
            pltpu.VMEM((n, 2, block, LANES), F32),
            pltpu.VMEM((pieces, 3, block, LANES), F32),
            dma((slab,)), dma((2,)), pltpu.SemaphoreType.REGULAR,
            dma, dma((n_col,)), dma, dma, dma((halves, share)), dma((halves, share)),
            dma((halves, share)), dma((halves, share)), dma((halves,)), dma((halves,)), dma((halves,)), dma((halves,)),
        ],
        compiler_params=pltpu.CompilerParams(
            collective_id=0, has_side_effects=True, vmem_limit_bytes=40 * 2**20
        ),
        name="project_and_gram",
    )(*(pltpu.with_memory_space_constraint(x, pltpu.HBM) for x in (tensor, factor_one, factor_two.T)))
    return gram


def solution(mesh):
    sizes = mesh.shape
    placed = (P(("row", "col"), None, None), P(("row", "col"), None), P("col", None))
    return jax.shard_map(
        functools.partial(per_device, sizes["row"], sizes["col"]),
        mesh=mesh, in_specs=placed, out_specs=P(), check_vma=False,
    )
```
